32 devices in a mesh: groups: 2 (over y), gx: 16 (over z, x, core).
Axes of the slice: x: 2, y: 2, z: 4, core: 2. Of those that a mesh axis runs over, the one named last changes fastest.
Arguments:
- pressure: float32 [7, 256, 128, 128], P(None, ('groups', 'gx')), parts along dimension 1, may hold values from -6 to 6
- adjoint: float32 [7, 256, 128, 128], P(None, ('groups', 'gx')), parts along dimension 1, may hold values from -6 to 6
- permeability: float32 [3, 256, 128, 128], P(None, ('groups', 'gx')), parts along dimension 1, may hold values from 0.02 to 40, as said below
- active: int32 [256, 128, 128], P(('groups', 'gx')), parts along dimension 0, may hold values 0 or 1
- fault_codes: int32 [3, 256, 128, 128], P(None, ('groups', 'gx')), parts along dimension 1, may hold values from 0 to 3
Outputs:
- gradient: float32 [3, 256, 128, 128], P(None, ('groups', 'gx')), parts along dimension 1
The draws below stay inside these ranges and needn't reach their ends.
There are 2 independent parts, one for each index of `groups`. The reference program is written for one: setup_inputs(seed, part) draws one part's arguments, and reference() takes and returns one part's arrays. A program takes and returns all parts, laid end to end along the dimension named above; each array names one. Nothing has to cross between parts.
Inputs may be any that keep to these rules, and one draw needn't show every extreme that they name: `permeability`: Positive.
All inputs are finite; a program needn't handle non-finite values. No bound on the sum of `active` on one device may be relied on, other than what follows from the above.
Results may differ from the reference program's by a relative error of at most 0.0003.
Values sent between devices are 32-bit elements; how exact they have to be, the bound alone decides.
A program may use at most 64 MiB of HBM per device.

```python
import jax
import jax.numpy as jnp
from jax import lax

NT = 7
NY = 128
NZ = 128
NX = 128


def draw_permeability(key, part):
    shape = (3, NX, NY, NZ)
    position = jnp.arange(NX, dtype=jnp.float32) / NX
    rough = jnp.clip(0.7 * jax.random.normal(key, shape, jnp.float32), -2.1, 2.1)
    trend = 1.0 + 2.0 * position
    aniso = jnp.array([1.0, 1.0, 0.2], jnp.float32).reshape(3, 1, 1, 1)
    return (aniso * jnp.exp(rough) * trend[None, :, None, None]).astype(jnp.float32)


def plant(values, stream_key, least, high):
    longest = values.shape.index(max(values.shape))
    spots = []
    for shift in (0, 1):
        where = [jax.random.randint(jax.random.fold_in(stream_key, axis), (), 0, length) for axis, length in enumerate(values.shape)]
        where[longest] = (where[longest] + shift) % values.shape[longest]
        spots.append(tuple(where))
    return values.at[spots[0]].set(least).at[spots[1]].set(high)


def steps_of(rng, dims, split, least, high):
    level, own = 1.0, jax.random.fold_in(rng, 6)
    for axis_at, parts in split:
        steps = jnp.exp(jax.random.uniform(jax.random.fold_in(own, axis_at), (parts,), jnp.float32, least / len(split), high / len(split)))
        level = level * jnp.repeat(steps, dims[axis_at] // parts).reshape([-1 if axis == axis_at else 1 for axis in range(len(dims))])
    return level


def scatter_about(key, extent, width, reach, split=(), kind=jnp.bfloat16):
    drawn = jax.random.normal(key, extent, jnp.float32) * width
    if len(split) > 0:
        drawn = steps_of(key, extent, split, -0.22, 0.18) * drawn
    return jnp.clip(drawn, min=-reach, max=reach).astype(kind)


def setup_inputs(seed: int = 0, part: int = 0) -> dict:
    splits = jax.random.split(jax.random.key(seed), 6)
    part_splits = jax.random.split(jax.random.fold_in(splits[5], part), 6)
    return {
        "pressure": scatter_about(part_splits[0], (NT, NX, NY, NZ), 1.0, 6.0, ((1, 16),), jnp.float32),
        "adjoint": scatter_about(part_splits[1], (NT, NX, NY, NZ), 1.0, 6.0, ((1, 16),), jnp.float32),
        "permeability": draw_permeability(jax.random.fold_in(jax.random.fold_in(splits[5], part), 71), part),
        "active": plant((jax.random.randint(part_splits[3], (NX, NY, NZ), 0, 10) < 9).astype(jnp.int32), jax.random.fold_in(part_splits[3], 1), 0, 1),
        "fault_codes": plant(jax.random.randint(part_splits[4], (3, NX, NY, NZ), 0, 4), jax.random.fold_in(part_splits[4], 1), 0, 3).astype(jnp.int32),
    }


epsilon = 1e-06

def multiplier(codes):
    return jnp.where(codes == 0, 1.0, jnp.where(codes == 1, 0.6, jnp.where(codes == 2, 0.25, 0.05))).astype(jnp.float32)

def pair_terms(lower_pres, upper_pres, lower_adj, upper_adj, lower_perm, upper_perm, factor):
    products = lax.optimization_barrier(jnp.sum((lower_adj - upper_adj) * (lower_pres - upper_pres), axis=0))
    summed = lower_perm + upper_perm
    scaled = 2.0 * factor * products / (summed * summed)
    return (scaled * upper_perm * upper_perm, scaled * lower_perm * lower_perm)

def cut(values, start, stop, along):
    return lax.slice_in_dim(values, start, stop, axis=along)

def direction_grad(pressure, adjoint, perm_dir, opened, codes, along):
    count = opened.shape[along]
    factor = multiplier(cut(codes, 0, count - 1, along)) * cut(opened, 0, count - 1, along) * cut(opened, 1, count, along)
    to_lower, to_upper = pair_terms(cut(pressure, 0, count - 1, along + 1), cut(pressure, 1, count, along + 1), cut(adjoint, 0, count - 1, along + 1), cut(adjoint, 1, count, along + 1), cut(perm_dir, 0, count - 1, along), cut(perm_dir, 1, count, along), factor)
    widths_lower = [(0, 0), (0, 0), (0, 0)]
    widths_upper = [(0, 0), (0, 0), (0, 0)]
    widths_lower[along] = (0, 1)
    widths_upper[along] = (1, 0)
    return jnp.pad(to_lower, widths_lower) + jnp.pad(to_upper, widths_upper)

def reference(pressure, adjoint, permeability, active, fault_codes):
    opened = active.astype(jnp.float32)
    logs = []
    for direction in range(3):
        grad = direction_grad(pressure, adjoint, permeability[direction], opened, fault_codes[direction], direction)
        logs.append(permeability[direction] * grad)
    stacked = jnp.stack(logs)
    total = jnp.sum(stacked * stacked)
    root_mean = jnp.sqrt(total / (3 * NX * NY * NZ) + epsilon)
    return stacked / root_mean
```

```python
import functools

import jax
import jax.numpy as jnp
from jax import lax
from jax.experimental import pallas as pl
from jax.experimental.pallas import tpu as pltpu
from jax.sharding import PartitionSpec as P

MESH = pl.DeviceIdType.MESH
epsilon = 1e-06
ROWS = 32
PAD = 8


def multiplier(codes):
    return jnp.where(codes == 0, 1.0, jnp.where(codes == 1, 0.6, jnp.where(codes == 2, 0.25, 0.05))).astype(jnp.float32)


def fold(values):
    squares = values * values
    total = squares[0:8]
    for i in range(8, squares.shape[0], 8):
        total = total + squares[i : i + 8]
    return total


def weight(products, factor, k_lo, k_up):
    summed = k_lo + k_up
    return 2.0 * factor * products * (k_lo * k_up) / (summed * summed)


def kernel(
    n, entries, p_hbm, a_hbm, k_hbm, act_hbm, code_hbm, grad, scale,
    p, a, k, act, code, halo_p, halo_a, halo_g, g_out, ret_out, ret_in, tail, part, parts,
    load_sem, halo_send, halo_recv, ret_send, ret_recv, part_send, part_recv,
):
    me = lax.axis_index("gx")
    lower, upper = me - 1, me + 1
    steps, layers, height, width = p_hbm.shape
    last = layers - 1
    blocks = height // ROWS

    barrier = pltpu.get_barrier_semaphore()

    def greet(j, carry):
        pl.semaphore_signal(barrier, inc=1, device_id={"gx": lax.rem(me + j, n)}, device_id_type=MESH)
        return carry

    lax.fori_loop(1, n, greet, 0)

    def loads(l):
        return (
            pltpu.make_async_copy(k_hbm.at[:, l], k.at[:, l, pl.ds(0, height)], load_sem.at[2, l]),
            pltpu.make_async_copy(act_hbm.at[l], act.at[l, pl.ds(0, height)], load_sem.at[3, l]),
            pltpu.make_async_copy(code_hbm.at[:, l], code.at[:, l], load_sem.at[4, l]),
            pltpu.make_async_copy(p_hbm.at[:, l], p.at[:, l, pl.ds(0, height)], load_sem.at[0, l]),
            pltpu.make_async_copy(a_hbm.at[:, l], a.at[:, l, pl.ds(0, height)], load_sem.at[1, l]),
        )

    def halo_pa(c):
        rows = pl.ds(c * ROWS, ROWS)
        return (
            pltpu.make_async_remote_copy(
                src_ref=p_hbm.at[:, 0, rows], dst_ref=halo_p.at[:, rows],
                send_sem=halo_send.at[2 * c], recv_sem=halo_recv.at[2 * c],
                device_id={"gx": lower}, device_id_type=MESH),
            pltpu.make_async_remote_copy(
                src_ref=a_hbm.at[:, 0, rows], dst_ref=halo_a.at[:, rows],
                send_sem=halo_send.at[2 * c + 1], recv_sem=halo_recv.at[2 * c + 1],
                device_id={"gx": lower}, device_id_type=MESH),
        )

    halo_k = pltpu.make_async_remote_copy(
        src_ref=g_out, dst_ref=halo_g, send_sem=halo_send.at[2 * blocks], recv_sem=halo_recv.at[2 * blocks],
        device_id={"gx": lower}, device_id_type=MESH)

    def returned(c):
        rows = pl.ds(c * ROWS, ROWS)
        return pltpu.make_async_remote_copy(
            src_ref=ret_out.at[rows], dst_ref=ret_in.at[rows], send_sem=ret_send.at[c], recv_sem=ret_recv.at[c],
            device_id={"gx": upper}, device_id_type=MESH)

    first = loads(0)
    for copy in first[:3]:
        copy.start()

    pl.semaphore_wait(barrier, n - 1)

    @pl.when(me > 0)
    def _():
        for copy in halo_pa(0):
            copy.start()

    for copy in first[3:]:
        copy.start()

    def start_layer(l, carry):
        for copy in loads(l):
            copy.start()
        return carry

    lax.fori_loop(1, layers, start_layer, 0)
    for copy in first[:2]:
        copy.wait()
    g_out[...] = k[0, 0, 0:height] * act[0, 0:height].astype(jnp.float32)

    @pl.when(me > 0)
    def _():
        halo_k.start()
        for c in range(1, blocks):
            for copy in halo_pa(c):
                copy.start()

    for copy in first[2:]:
        copy.wait()
    tail[0:8] = jnp.zeros((8, width), jnp.float32)
    lane = lax.broadcasted_iota(jnp.int32, (ROWS, width), 1)
    row = lax.broadcasted_iota(jnp.int32, (ROWS, width), 0)
    grad[0, 0] = jnp.zeros((height, width), jnp.float32)

    def layer(l, total):
        @pl.when(l < last)
        def _():
            for copy in loads(l + 1):
                copy.wait()

        def block(b, total):
            r = pl.multiple_of(b * ROWS, ROWS)
            here, after = pl.ds(r, ROWS), pl.ds(r + 1, ROWS)
            prod_y = jnp.zeros((ROWS, width), jnp.float32)
            prod_z = jnp.zeros((ROWS, width), jnp.float32)
            for t in range(steps):
                pt, at = p[t, l, here], a[t, l, here]
                prod_y += (at - a[t, l, after]) * (pt - p[t, l, after])
                prod_z += (at - pltpu.roll(at, width - 1, 1)) * (pt - pltpu.roll(pt, width - 1, 1))
            opened = act[l, here].astype(jnp.float32)
            k1 = k[1, l, here]
            k1_up = k[1, l, after]
            factor = multiplier(code[1, l, here]) * opened * act[l, after].astype(jnp.float32)
            w = jnp.where(row + r < height - 1, weight(prod_y, factor, k1, k1_up), 0.0)
            w_lo = jnp.where(row + r < height - 1, w * k1_up, 0.0)
            tail[pl.ds(r + 8, ROWS)] = w * k1
            log1 = w_lo + tail[pl.ds(r + 7, ROWS)]
            grad[1, l, here] = log1
            k2 = k[2, l, here]
            k2_up = pltpu.roll(k2, width - 1, 1)
            factor = multiplier(code[2, l, here]) * opened * pltpu.roll(opened, width - 1, 1)
            w = jnp.where(lane < width - 1, weight(prod_z, factor, k2, k2_up), 0.0)
            log2 = w * k2_up + pltpu.roll(w * k2, 1, 1)
            grad[2, l, here] = log2
            return total + fold(log1) + fold(log2)

        total = lax.fori_loop(0, blocks, block, total)

        def cross(b, total):
            here = pl.ds(pl.multiple_of(b * ROWS, ROWS), ROWS)
            prod = jnp.zeros((ROWS, width), jnp.float32)
            for t in range(steps):
                prod += (a[t, l, here] - a[t, l + 1, here]) * (p[t, l, here] - p[t, l + 1, here])
            k0, k0_up = k[0, l, here], k[0, l + 1, here]
            factor = multiplier(code[0, l, here]) * (act[l, here] * act[l + 1, here]).astype(jnp.float32)
            w = weight(prod, factor, k0, k0_up)
            log0 = grad[0, l, here] + w * k0_up
            grad[0, l, here] = log0
            grad[0, l + 1, here] = w * k0
            return total + jnp.where(l > 0, 1.0, 0.0) * fold(log0)

        return lax.cond(l < last, lambda total: lax.fori_loop(0, blocks, cross, total), lambda total: total, total)

    total = lax.fori_loop(0, layers, layer, jnp.zeros((8, width), jnp.float32))
    part[...] = total

    @pl.when(me < n - 1)
    def _():
        halo_k.wait_recv()
        for c in range(blocks):
            for copy in halo_pa(c):
                copy.wait_recv()
            here = pl.ds(c * ROWS, ROWS)
            prod = jnp.zeros((ROWS, width), jnp.float32)
            for t in range(steps):
                prod += (a[t, last, here] - halo_a[t, here]) * (p[t, last, here] - halo_p[t, here])
            k0, g_up = k[0, last, here], halo_g[here]
            factor = multiplier(code[0, last, here]) * act[last, here].astype(jnp.float32)
            w = weight(prod, factor, k0, g_up)
            ret_out[here] = w * k0
            returned(c).start()
            grad[0, last, here] = grad[0, last, here] + w * g_up

    part[...] = part[...] + fold(grad[0, last])

    @pl.when(me > 0)
    def _():
        for c in range(blocks):
            here = pl.ds(c * ROWS, ROWS)
            returned(c).wait_recv()
            grad[0, 0, here] = grad[0, 0, here] + ret_in[here]

    part[...] = part[...] + fold(grad[0, 0])

    def to_peer(j):
        return pltpu.make_async_remote_copy(
            src_ref=part, dst_ref=parts.at[j - 1], send_sem=part_send.at[j - 1], recv_sem=part_recv.at[j - 1],
            device_id={"gx": lax.rem(me + j, n)}, device_id_type=MESH)

    def send(j, carry):
        to_peer(j).start()
        return carry

    def receive(j, carry):
        to_peer(j).wait_recv()
        return carry

    lax.fori_loop(1, n, send, 0)
    lax.fori_loop(1, n, receive, 0)
    whole = jnp.sum(jnp.sum(parts[...], axis=0) + part[...], keepdims=True)
    scale[...] = jnp.broadcast_to(lax.rsqrt(whole / entries + epsilon), scale.shape)

    def drain(j, carry):
        to_peer(j).wait_send()
        return carry

    lax.fori_loop(1, n, drain, 0)

    @pl.when(me > 0)
    def _():
        halo_k.wait_send()
        for c in range(blocks):
            for copy in halo_pa(c):
                copy.wait_send()

    @pl.when(me < n - 1)
    def _():
        for c in range(blocks):
            returned(c).wait_send()


def local(pressure, adjoint, permeability, active, fault_codes):
    n = lax.axis_size("gx")
    steps, layers, height, width = pressure.shape
    blocks = height // ROWS
    entries = 3 * layers * n * height * width
    f32 = jnp.float32
    padded = height + PAD
    dma = pltpu.SemaphoreType.DMA
    grad, scale = pl.pallas_call(
        functools.partial(kernel, n, entries),
        out_shape=(
            jax.ShapeDtypeStruct((3, layers, height, width), f32),
            jax.ShapeDtypeStruct((8, width), f32),
        ),
        in_specs=[pl.BlockSpec(memory_space=pltpu.HBM)] * 5,
        out_specs=(pl.BlockSpec(memory_space=pltpu.VMEM), pl.BlockSpec(memory_space=pltpu.VMEM)),
        scratch_shapes=[
            pltpu.VMEM((steps, layers, padded, width), f32),
            pltpu.VMEM((steps, layers, padded, width), f32),
            pltpu.VMEM((3, layers, padded, width), f32),
            pltpu.VMEM((layers, padded, width), jnp.int32),
            pltpu.VMEM((3, layers, height, width), jnp.int32),
            pltpu.VMEM((steps, height, width), f32),
            pltpu.VMEM((steps, height, width), f32),
            pltpu.VMEM((height, width), f32),
            pltpu.VMEM((height, width), f32),
            pltpu.VMEM((height, width), f32),
            pltpu.VMEM((height, width), f32),
            pltpu.VMEM((padded, width), f32),
            pltpu.VMEM((8, width), f32),
            pltpu.VMEM((n - 1, 8, width), f32),
            dma((5, layers)),
            dma((2 * blocks + 1,)),
            dma((2 * blocks + 1,)),
            dma((blocks,)),
            dma((blocks,)),
            dma((n - 1,)),
            dma((n - 1,)),
        ],
        compiler_params=pltpu.CompilerParams(collective_id=0, has_side_effects=True, vmem_limit_bytes=40 * 1024 * 1024),
        cost_estimate=pl.CostEstimate(flops=100_000_000, bytes_accessed=12_000_000, transcendentals=0),
    )(pressure, adjoint, permeability, active, fault_codes)
    return grad * scale[0, 0]


def solution(mesh):
    split = ("groups", "gx")
    placed = (P(None, split), P(None, split), P(None, split), P(split), P(None, split))
    return jax.shard_map(local, mesh=mesh, in_specs=placed, out_specs=P(None, split), check_vma=False)
```

```python
import functools

import jax
import jax.numpy as jnp
from jax import lax
from jax.experimental import pallas as pl
from jax.experimental.pallas import tpu as pltpu
from jax.sharding import PartitionSpec as P

MESH = pl.DeviceIdType.MESH
epsilon = 1e-06
ROWS = 32
PAD = 8


def multiplier(codes):
    return jnp.where(codes == 0, 1.0, jnp.where(codes == 1, 0.6, jnp.where(codes == 2, 0.25, 0.05))).astype(jnp.float32)


def fold(values):
    squares = values * values
    total = squares[0:8]
    for i in range(8, squares.shape[0], 8):
        total = total + squares[i : i + 8]
    return total


def weight(products, factor, k_lo, k_up):
    summed = k_lo + k_up
    return 2.0 * factor * products * (k_lo * k_up) / (summed * summed)


def kernel(
    n, entries, p_hbm, a_hbm, k_hbm, act_hbm, code_hbm, out_hbm, scale,
    p, a, k, act, code, grad, halo_p, halo_a, halo_g, halo_own, g_out, ret_out, ret_in, tail, part, parts,
    load_sem, out_sem, halo_send, halo_recv, ret_send, ret_recv, part_send, part_recv,
):
    me = lax.axis_index("gx")
    lower, upper = me - 1, me + 1
    steps, layers, height, width = p_hbm.shape
    last = layers - 1
    blocks = height // ROWS

    barrier = pltpu.get_barrier_semaphore()

    def greet(j, carry):
        pl.semaphore_signal(barrier, inc=1, device_id={"gx": lax.rem(me + j, n)}, device_id_type=MESH)
        return carry

    lax.fori_loop(1, n, greet, 0)

    def loads(l):
        return (
            pltpu.make_async_copy(k_hbm.at[:, l], k.at[:, l, pl.ds(0, height)], load_sem.at[2, l]),
            pltpu.make_async_copy(act_hbm.at[l], act.at[l, pl.ds(0, height)], load_sem.at[3, l]),
            pltpu.make_async_copy(code_hbm.at[:, l], code.at[:, l], load_sem.at[4, l]),
            pltpu.make_async_copy(p_hbm.at[:, l], p.at[:, l, pl.ds(0, height)], load_sem.at[0, l]),
            pltpu.make_async_copy(a_hbm.at[:, l], a.at[:, l, pl.ds(0, height)], load_sem.at[1, l]),
        )

    def halo_pa(c):
        rows = pl.ds(c * ROWS, ROWS)
        return (
            pltpu.make_async_remote_copy(
                src_ref=p_hbm.at[:, 0, rows], dst_ref=halo_p.at[:, rows],
                send_sem=halo_send.at[2 * c], recv_sem=halo_recv.at[2 * c],
                device_id={"gx": lower}, device_id_type=MESH),
            pltpu.make_async_remote_copy(
                src_ref=a_hbm.at[:, 0, rows], dst_ref=halo_a.at[:, rows],
                send_sem=halo_send.at[2 * c + 1], recv_sem=halo_recv.at[2 * c + 1],
                device_id={"gx": lower}, device_id_type=MESH),
        )

    halo_k = pltpu.make_async_remote_copy(
        src_ref=g_out, dst_ref=halo_g, send_sem=halo_send.at[2 * blocks], recv_sem=halo_recv.at[2 * blocks],
        device_id={"gx": lower}, device_id_type=MESH)

    halo_first = pltpu.make_async_remote_copy(
        src_ref=grad.at[0, 0], dst_ref=halo_own, send_sem=halo_send.at[2 * blocks + 1], recv_sem=halo_recv.at[2 * blocks + 1],
        device_id={"gx": lower}, device_id_type=MESH)

    def written(d, l):
        return pltpu.make_async_copy(grad.at[d, l], out_hbm.at[d, l], out_sem.at[d, l])

    def returned(c):
        rows = pl.ds(c * ROWS, ROWS)
        return pltpu.make_async_remote_copy(
            src_ref=ret_out.at[rows], dst_ref=ret_in.at[rows], send_sem=ret_send.at[c], recv_sem=ret_recv.at[c],
            device_id={"gx": upper}, device_id_type=MESH)

    first = loads(0)
    for copy in first[:3]:
        copy.start()

    pl.semaphore_wait(barrier, n - 1)

    @pl.when(me > 0)
    def _():
        for c in range(blocks // 2):
            for copy in halo_pa(c):
                copy.start()

    for copy in first[3:]:
        copy.start()

    def start_layer(l, carry):
        for copy in loads(l):
            copy.start()
        return carry

    lax.fori_loop(1, layers, start_layer, 0)
    for copy in first[:2]:
        copy.wait()
    g_out[...] = k[0, 0, 0:height] * act[0, 0:height].astype(jnp.float32)

    @pl.when(me > 0)
    def _():
        halo_k.start()

    for copy in first[2:]:
        copy.wait()
    tail[0:8] = jnp.zeros((8, width), jnp.float32)
    lane = lax.broadcasted_iota(jnp.int32, (ROWS, width), 1)
    row = lax.broadcasted_iota(jnp.int32, (ROWS, width), 0)
    grad[0, 0] = jnp.zeros((height, width), jnp.float32)

    def layer(l, total):
        @pl.when(l < last)
        def _():
            for copy in loads(l + 1):
                copy.wait()

        @pl.when(jnp.logical_and(l == 1, me > 0))
        def _():
            halo_first.start()
            for c in range(blocks // 2, blocks):
                for copy in halo_pa(c):
                    copy.start()

        def block(b, total):
            r = pl.multiple_of(b * ROWS, ROWS)
            here, after = pl.ds(r, ROWS), pl.ds(r + 1, ROWS)
            prod_y = jnp.zeros((ROWS, width), jnp.float32)
            prod_z = jnp.zeros((ROWS, width), jnp.float32)
            for t in range(steps):
                pt, at = p[t, l, here], a[t, l, here]
                prod_y += (at - a[t, l, after]) * (pt - p[t, l, after])
                prod_z += (at - pltpu.roll(at, width - 1, 1)) * (pt - pltpu.roll(pt, width - 1, 1))
            opened = act[l, here].astype(jnp.float32)
            k1 = k[1, l, here]
            k1_up = k[1, l, after]
            factor = multiplier(code[1, l, here]) * opened * act[l, after].astype(jnp.float32)
            w = jnp.where(row + r < height - 1, weight(prod_y, factor, k1, k1_up), 0.0)
            w_lo = jnp.where(row + r < height - 1, w * k1_up, 0.0)
            tail[pl.ds(r + 8, ROWS)] = w * k1
            log1 = w_lo + tail[pl.ds(r + 7, ROWS)]
            grad[1, l, here] = log1
            k2 = k[2, l, here]
            k2_up = pltpu.roll(k2, width - 1, 1)
            factor = multiplier(code[2, l, here]) * opened * pltpu.roll(opened, width - 1, 1)
            w = jnp.where(lane < width - 1, weight(prod_z, factor, k2, k2_up), 0.0)
            log2 = w * k2_up + pltpu.roll(w * k2, 1, 1)
            grad[2, l, here] = log2
            return total + fold(log1) + fold(log2)

        total = lax.fori_loop(0, blocks, block, total)

        def cross(b, total):
            here = pl.ds(pl.multiple_of(b * ROWS, ROWS), ROWS)
            prod = jnp.zeros((ROWS, width), jnp.float32)
            for t in range(steps):
                prod += (a[t, l, here] - a[t, l + 1, here]) * (p[t, l, here] - p[t, l + 1, here])
            k0, k0_up = k[0, l, here], k[0, l + 1, here]
            factor = multiplier(code[0, l, here]) * (act[l, here] * act[l + 1, here]).astype(jnp.float32)
            w = weight(prod, factor, k0, k0_up)
            log0 = grad[0, l, here] + w * k0_up
            grad[0, l, here] = log0
            grad[0, l + 1, here] = w * k0
            return total + jnp.where(l > 0, 1.0, 0.0) * fold(log0)

        written(1, l).start()
        written(2, l).start()
        total = lax.cond(l < last, lambda total: lax.fori_loop(0, blocks, cross, total), lambda total: total, total)

        @pl.when(jnp.logical_and(l > 0, l < last))
        def _():
            written(0, l).start()

        return total

    total = lax.fori_loop(0, layers, layer, jnp.zeros((8, width), jnp.float32))
    part[...] = total + jnp.where(me == 0, 1.0, 0.0) * fold(grad[0, 0])

    @pl.when(me < n - 1)
    def _():
        halo_k.wait_recv()
        halo_first.wait_recv()
        for c in range(blocks):
            for copy in halo_pa(c):
                copy.wait_recv()
            here = pl.ds(c * ROWS, ROWS)
            prod = jnp.zeros((ROWS, width), jnp.float32)
            for t in range(steps):
                prod += (a[t, last, here] - halo_a[t, here]) * (p[t, last, here] - halo_p[t, here])
            k0, g_up = k[0, last, here], halo_g[here]
            factor = multiplier(code[0, last, here]) * act[last, here].astype(jnp.float32)
            w = weight(prod, factor, k0, g_up)
            w_up = w * k0
            ret_out[here] = w_up
            returned(c).start()
            grad[0, last, here] = grad[0, last, here] + w * g_up
            part[...] = part[...] + fold(halo_own[here] + w_up)

    part[...] = part[...] + fold(grad[0, last])

    def to_peer(j):
        return pltpu.make_async_remote_copy(
            src_ref=part, dst_ref=parts.at[j - 1], send_sem=part_send.at[j - 1], recv_sem=part_recv.at[j - 1],
            device_id={"gx": lax.rem(me + j, n)}, device_id_type=MESH)

    def send(j, carry):
        to_peer(j).start()
        return carry

    def receive(j, carry):
        to_peer(j).wait_recv()
        return carry

    lax.fori_loop(1, n, send, 0)
    written(0, last).start()

    @pl.when(me > 0)
    def _():
        halo_first.wait_send()
        for c in range(blocks):
            here = pl.ds(c * ROWS, ROWS)
            returned(c).wait_recv()
            grad[0, 0, here] = grad[0, 0, here] + ret_in[here]

    written(0, 0).start()
    lax.fori_loop(1, n, receive, 0)
    whole = jnp.sum(jnp.sum(parts[...], axis=0) + part[...], keepdims=True)
    scale[...] = jnp.broadcast_to(lax.rsqrt(whole / entries + epsilon), scale.shape)

    def drain(j, carry):
        to_peer(j).wait_send()
        return carry

    lax.fori_loop(1, n, drain, 0)

    @pl.when(me > 0)
    def _():
        halo_k.wait_send()
        for c in range(blocks):
            for copy in halo_pa(c):
                copy.wait_send()

    @pl.when(me < n - 1)
    def _():
        for c in range(blocks):
            returned(c).wait_send()

    def finish(l, carry):
        for d in range(3):
            written(d, l).wait()
        return carry

    lax.fori_loop(0, layers, finish, 0)


def local(pressure, adjoint, permeability, active, fault_codes):
    n = lax.axis_size("gx")
    steps, layers, height, width = pressure.shape
    blocks = height // ROWS
    entries = 3 * layers * n * height * width
    f32 = jnp.float32
    padded = height + PAD
    dma = pltpu.SemaphoreType.DMA
    grad, scale = pl.pallas_call(
        functools.partial(kernel, n, entries),
        out_shape=(
            jax.ShapeDtypeStruct((3, layers, height, width), f32),
            jax.ShapeDtypeStruct((height, width), f32),
        ),
        in_specs=[pl.BlockSpec(memory_space=pltpu.HBM)] * 5,
        out_specs=(pl.BlockSpec(memory_space=pltpu.HBM), pl.BlockSpec(memory_space=pltpu.VMEM)),
        scratch_shapes=[
            pltpu.VMEM((steps, layers, padded, width), f32),
            pltpu.VMEM((steps, layers, padded, width), f32),
            pltpu.VMEM((3, layers, padded, width), f32),
            pltpu.VMEM((layers, padded, width), jnp.int32),
            pltpu.VMEM((3, layers, height, width), jnp.int32),
            pltpu.VMEM((3, layers, height, width), f32),
            pltpu.VMEM((steps, height, width), f32),
            pltpu.VMEM((steps, height, width), f32),
            pltpu.VMEM((height, width), f32),
            pltpu.VMEM((height, width), f32),
            pltpu.VMEM((height, width), f32),
            pltpu.VMEM((height, width), f32),
            pltpu.VMEM((height, width), f32),
            pltpu.VMEM((padded, width), f32),
            pltpu.VMEM((8, width), f32),
            pltpu.VMEM((n - 1, 8, width), f32),
            dma((5, layers)),
            dma((3, layers)),
            dma((2 * blocks + 2,)),
            dma((2 * blocks + 2,)),
            dma((blocks,)),
            dma((blocks,)),
            dma((n - 1,)),
            dma((n - 1,)),
        ],
        compiler_params=pltpu.CompilerParams(collective_id=0, has_side_effects=True, vmem_limit_bytes=60 * 1024 * 1024),
        cost_estimate=pl.CostEstimate(flops=100_000_000, bytes_accessed=12_000_000, transcendentals=0),
    )(pressure, adjoint, permeability, active, fault_codes)
    return grad * scale


def solution(mesh):
    split = ("groups", "gx")
    placed = (P(None, split), P(None, split), P(None, split), P(split), P(None, split))
    return jax.shard_map(local, mesh=mesh, in_specs=placed, out_specs=P(None, split), check_vma=False)
```

```python
import functools

import jax
import jax.numpy as jnp
from jax import lax
from jax.experimental import pallas as pl
from jax.experimental.pallas import tpu as pltpu
from jax.sharding import PartitionSpec as P

MESH = pl.DeviceIdType.MESH
epsilon = 1e-06
ROWS = 32
PAD = 8
GRANT = 58_000_000


def multiplier(codes):
    return jnp.where(codes == 0, 1.0, jnp.where(codes == 1, 0.6, jnp.where(codes == 2, 0.25, 0.05))).astype(jnp.float32)


def fold(values):
    squares = values * values
    total = squares[0:8]
    for i in range(8, squares.shape[0], 8):
        total = total + squares[i : i + 8]
    return total


def weight(products, factor, k_lo, k_up):
    summed = k_lo + k_up
    return 2.0 * factor * products * (k_lo * k_up) / (summed * summed)


def distances(n):
    reach, rounds = 1, []
    while reach < n - 1:
        rounds.append(reach)
        reach *= 2
    return rounds


def kernel(
    n, entries, p_hbm, a_hbm, k_hbm, act_hbm, code_hbm, grad,
    p, a, k, act, code, halo_p, halo_a, halo_g, halo_own, g_out, ret_out, ret_in, tail, part, parts,
    load_sem, halo_send, halo_recv, ret_send, ret_recv, part_send, part_recv, near_sem,
):
    me = lax.axis_index("gx")
    lower, upper = me - 1, me + 1
    steps, layers, height, width = p_hbm.shape
    last = layers - 1
    blocks = height // ROWS

    barrier = pltpu.get_barrier_semaphore()

    def signal(semaphore, distance):
        for there, inside in ((me - distance, me >= distance), (me + distance, me + distance < n)):
            @pl.when(inside)
            def _():
                pl.semaphore_signal(semaphore, inc=1, device_id={"gx": there}, device_id_type=MESH)

    def await_signals(semaphore, distance):
        peers = jnp.where(me >= distance, 1, 0) + jnp.where(me + distance < n, 1, 0)
        pl.semaphore_wait(semaphore, peers)

    signal(barrier, 1)

    def loads(l):
        return (
            pltpu.make_async_copy(k_hbm.at[:, l], k.at[:, l, pl.ds(0, height)], load_sem.at[2, l]),
            pltpu.make_async_copy(act_hbm.at[l], act.at[l, pl.ds(0, height)], load_sem.at[3, l]),
            pltpu.make_async_copy(code_hbm.at[:, l], code.at[:, l], load_sem.at[4, l]),
            pltpu.make_async_copy(p_hbm.at[:, l], p.at[:, l, pl.ds(0, height)], load_sem.at[0, l]),
            pltpu.make_async_copy(a_hbm.at[:, l], a.at[:, l, pl.ds(0, height)], load_sem.at[1, l]),
        )

    def halo_pa(c):
        rows = pl.ds(c * ROWS, ROWS)
        return (
            pltpu.make_async_remote_copy(
                src_ref=p_hbm.at[:, 0, rows], dst_ref=halo_p.at[:, rows],
                send_sem=halo_send.at[2 * c], recv_sem=halo_recv.at[2 * c],
                device_id={"gx": lower}, device_id_type=MESH),
            pltpu.make_async_remote_copy(
                src_ref=a_hbm.at[:, 0, rows], dst_ref=halo_a.at[:, rows],
                send_sem=halo_send.at[2 * c + 1], recv_sem=halo_recv.at[2 * c + 1],
                device_id={"gx": lower}, device_id_type=MESH),
        )

    halo_k = pltpu.make_async_remote_copy(
        src_ref=g_out, dst_ref=halo_g, send_sem=halo_send.at[2 * blocks], recv_sem=halo_recv.at[2 * blocks],
        device_id={"gx": lower}, device_id_type=MESH)

    halo_first = pltpu.make_async_remote_copy(
        src_ref=grad.at[0, 0], dst_ref=halo_own, send_sem=halo_send.at[2 * blocks + 1], recv_sem=halo_recv.at[2 * blocks + 1],
        device_id={"gx": lower}, device_id_type=MESH)

    def returned(c):
        rows = pl.ds(c * ROWS, ROWS)
        return pltpu.make_async_remote_copy(
            src_ref=ret_out.at[rows], dst_ref=ret_in.at[rows], send_sem=ret_send.at[c], recv_sem=ret_recv.at[c],
            device_id={"gx": upper}, device_id_type=MESH)

    first = loads(0)
    for copy in first[:3]:
        copy.start()

    await_signals(barrier, 1)

    @pl.when(me > 0)
    def _():
        for c in range(blocks // 2):
            for copy in halo_pa(c):
                copy.start()

    for copy in first[3:]:
        copy.start()

    def start_layer(l, carry):
        for copy in loads(l):
            copy.start()
        return carry

    lax.fori_loop(1, layers, start_layer, 0)
    for copy in first[:2]:
        copy.wait()
    g_out[...] = k[0, 0, 0:height] * act[0, 0:height].astype(jnp.float32)

    @pl.when(me > 0)
    def _():
        halo_k.start()

    for copy in first[2:]:
        copy.wait()
    tail[0:8] = jnp.zeros((8, width), jnp.float32)
    lane = lax.broadcasted_iota(jnp.int32, (ROWS, width), 1)
    row = lax.broadcasted_iota(jnp.int32, (ROWS, width), 0)
    grad[0, 0] = jnp.zeros((height, width), jnp.float32)

    def layer(l, total):
        @pl.when(l < last)
        def _():
            for copy in loads(l + 1):
                copy.wait()

        @pl.when(jnp.logical_and(l == 1, me > 0))
        def _():
            halo_first.start()
            for c in range(blocks // 2, blocks):
                for copy in halo_pa(c):
                    copy.start()

        def block(b, total):
            r = pl.multiple_of(b * ROWS, ROWS)
            here, after = pl.ds(r, ROWS), pl.ds(r + 1, ROWS)
            prod_y = jnp.zeros((ROWS, width), jnp.float32)
            prod_z = jnp.zeros((ROWS, width), jnp.float32)
            for t in range(steps):
                pt, at = p[t, l, here], a[t, l, here]
                prod_y += (at - a[t, l, after]) * (pt - p[t, l, after])
                prod_z += (at - pltpu.roll(at, width - 1, 1)) * (pt - pltpu.roll(pt, width - 1, 1))
            opened = act[l, here].astype(jnp.float32)
            k1 = k[1, l, here]
            k1_up = k[1, l, after]
            factor = multiplier(code[1, l, here]) * opened * act[l, after].astype(jnp.float32)
            w = jnp.where(row + r < height - 1, weight(prod_y, factor, k1, k1_up), 0.0)
            w_lo = jnp.where(row + r < height - 1, w * k1_up, 0.0)
            tail[pl.ds(r + 8, ROWS)] = w * k1
            log1 = w_lo + tail[pl.ds(r + 7, ROWS)]
            grad[1, l, here] = log1
            k2 = k[2, l, here]
            k2_up = pltpu.roll(k2, width - 1, 1)
            factor = multiplier(code[2, l, here]) * opened * pltpu.roll(opened, width - 1, 1)
            w = jnp.where(lane < width - 1, weight(prod_z, factor, k2, k2_up), 0.0)
            log2 = w * k2_up + pltpu.roll(w * k2, 1, 1)
            grad[2, l, here] = log2
            return total + fold(log1) + fold(log2)

        total = lax.fori_loop(0, blocks, block, total)

        def cross(b, total):
            here = pl.ds(pl.multiple_of(b * ROWS, ROWS), ROWS)
            prod = jnp.zeros((ROWS, width), jnp.float32)
            for t in range(steps):
                prod += (a[t, l, here] - a[t, l + 1, here]) * (p[t, l, here] - p[t, l + 1, here])
            k0, k0_up = k[0, l, here], k[0, l + 1, here]
            factor = multiplier(code[0, l, here]) * (act[l, here] * act[l + 1, here]).astype(jnp.float32)
            w = weight(prod, factor, k0, k0_up)
            log0 = grad[0, l, here] + w * k0_up
            grad[0, l, here] = log0
            grad[0, l + 1, here] = w * k0
            return total + jnp.where(l > 0, 1.0, 0.0) * fold(log0)

        return lax.cond(l < last, lambda total: lax.fori_loop(0, blocks, cross, total), lambda total: total, total)

    total = lax.fori_loop(0, layers, layer, jnp.zeros((8, width), jnp.float32))
    for i, distance in enumerate(distances(n)):
        signal(near_sem.at[i], distance)
        await_signals(near_sem.at[i], distance)

    part[...] = total + jnp.where(me == 0, 1.0, 0.0) * fold(grad[0, 0])

    @pl.when(me < n - 1)
    def _():
        halo_k.wait_recv()
        halo_first.wait_recv()
        for c in range(blocks):
            for copy in halo_pa(c):
                copy.wait_recv()
            here = pl.ds(c * ROWS, ROWS)
            prod = jnp.zeros((ROWS, width), jnp.float32)
            for t in range(steps):
                prod += (a[t, last, here] - halo_a[t, here]) * (p[t, last, here] - halo_p[t, here])
            k0, g_up = k[0, last, here], halo_g[here]
            factor = multiplier(code[0, last, here]) * act[last, here].astype(jnp.float32)
            w = weight(prod, factor, k0, g_up)
            w_up = w * k0
            ret_out[here] = w_up
            grad[0, last, here] = grad[0, last, here] + w * g_up
            part[...] = part[...] + fold(halo_own[here] + w_up)

    part[...] = part[...] + fold(grad[0, last])

    def to_peer(j):
        return pltpu.make_async_remote_copy(
            src_ref=part, dst_ref=parts.at[j - 1], send_sem=part_send.at[j - 1], recv_sem=part_recv.at[j - 1],
            device_id={"gx": lax.rem(me + j, n)}, device_id_type=MESH)

    def send(j, carry):
        to_peer(j).start()
        return carry

    def receive(j, carry):
        to_peer(j).wait_recv()
        return carry

    lax.fori_loop(1, n, send, 0)

    @pl.when(me < n - 1)
    def _():
        for c in range(blocks):
            returned(c).start()

    @pl.when(me > 0)
    def _():
        halo_first.wait_send()
        for c in range(blocks):
            here = pl.ds(c * ROWS, ROWS)
            returned(c).wait_recv()
            grad[0, 0, here] = grad[0, 0, here] + ret_in[here]

    lax.fori_loop(1, n, receive, 0)
    whole = jnp.sum(jnp.sum(parts[...], axis=0) + part[...], keepdims=True)
    scale = jnp.broadcast_to(lax.rsqrt(whole / entries + epsilon), (ROWS, width))

    def normalize(i, carry):
        here = pl.ds(pl.multiple_of(i * ROWS, ROWS), ROWS)
        for d in range(3):
            for l in range(layers):
                grad[d, l, here] = grad[d, l, here] * scale
        return carry

    lax.fori_loop(0, blocks, normalize, 0)

    def drain(j, carry):
        to_peer(j).wait_send()
        return carry

    lax.fori_loop(1, n, drain, 0)

    @pl.when(me > 0)
    def _():
        halo_k.wait_send()
        for c in range(blocks):
            for copy in halo_pa(c):
                copy.wait_send()

    @pl.when(me < n - 1)
    def _():
        for c in range(blocks):
            returned(c).wait_send()


def local(pressure, adjoint, permeability, active, fault_codes):
    n = lax.axis_size("gx")
    steps, layers, height, width = pressure.shape
    blocks = height // ROWS
    entries = 3 * layers * n * height * width
    f32 = jnp.float32
    padded = height + PAD
    dma = pltpu.SemaphoreType.DMA
    return pl.pallas_call(
        functools.partial(kernel, n, entries),
        out_shape=pltpu.VMEM((3, layers, height, width), f32),
        in_specs=[pl.BlockSpec(memory_space=pltpu.HBM)] * 5,
        out_specs=pl.BlockSpec(memory_space=pltpu.VMEM),
        scratch_shapes=[
            pltpu.VMEM((steps, layers, padded, width), f32),
            pltpu.VMEM((steps, layers, padded, width), f32),
            pltpu.VMEM((3, layers, padded, width), f32),
            pltpu.VMEM((layers, padded, width), jnp.int32),
            pltpu.VMEM((3, layers, height, width), jnp.int32),
            pltpu.VMEM((steps, height, width), f32),
            pltpu.VMEM((steps, height, width), f32),
            pltpu.VMEM((height, width), f32),
            pltpu.VMEM((height, width), f32),
            pltpu.VMEM((height, width), f32),
            pltpu.VMEM((height, width), f32),
            pltpu.VMEM((height, width), f32),
            pltpu.VMEM((padded, width), f32),
            pltpu.VMEM((8, width), f32),
            pltpu.VMEM((n - 1, 8, width), f32),
            dma((5, layers)),
            dma((2 * blocks + 2,)),
            dma((2 * blocks + 2,)),
            dma((blocks,)),
            dma((blocks,)),
            dma((n - 1,)),
            dma((n - 1,)),
            pltpu.SemaphoreType.REGULAR((len(distances(n)),)),
        ],
        compiler_params=pltpu.CompilerParams(collective_id=0, has_side_effects=True, vmem_limit_bytes=GRANT),
        cost_estimate=pl.CostEstimate(flops=100_000_000, bytes_accessed=12_000_000, transcendentals=0),
    )(pressure, adjoint, permeability, active, fault_codes)


def solution(mesh):
    split = ("groups", "gx")
    placed = (P(None, split), P(None, split), P(None, split), P(split), P(None, split))
    return jax.shard_map(local, mesh=mesh, in_specs=placed, out_specs=P(None, split), check_vma=False)
```

```python
import functools

import jax
import jax.numpy as jnp
from jax import lax
from jax.experimental import pallas as pl
from jax.experimental.pallas import tpu as pltpu
from jax.sharding import PartitionSpec as P

MESH = pl.DeviceIdType.MESH
epsilon = 1e-06
ROWS = 32
PAD = 8
GRANT = 58_000_000


def multiplier(codes):
    return jnp.where(codes == 0, 1.0, jnp.where(codes == 1, 0.6, jnp.where(codes == 2, 0.25, 0.05))).astype(jnp.float32)


def fold(values):
    squares = values * values
    total = squares[0:8]
    for i in range(8, squares.shape[0], 8):
        total = total + squares[i : i + 8]
    return total


def weight(products, factor, k_lo, k_up):
    summed = k_lo + k_up
    return 2.0 * factor * products * (k_lo * k_up) / (summed * summed)


def distances(n):
    reach, rounds = 1, []
    while reach < n - 1:
        rounds.append(reach)
        reach *= 2
    return rounds


def kernel(
    n, entries, p_hbm, a_hbm, k_hbm, act_hbm, code_hbm, grad,
    p, a, k, act, code, halo_p, halo_a, halo_g, halo_own, g_out, ret_out, ret_in, tail, acc, part, parts,
    load_sem, halo_send, halo_recv, ret_send, ret_recv, part_send, part_recv, near_sem,
):
    me = lax.axis_index("gx")
    lower, upper = me - 1, me + 1
    steps, layers, height, width = p_hbm.shape
    last = layers - 1
    blocks = height // ROWS

    barrier = pltpu.get_barrier_semaphore()

    def signal(semaphore, distance):
        for there, inside in ((me - distance, me >= distance), (me + distance, me + distance < n)):
            @pl.when(inside)
            def _():
                pl.semaphore_signal(semaphore, inc=1, device_id={"gx": there}, device_id_type=MESH)

    def await_signals(semaphore, distance):
        peers = jnp.where(me >= distance, 1, 0) + jnp.where(me + distance < n, 1, 0)
        pl.semaphore_wait(semaphore, peers)

    signal(barrier, 1)

    def loads(l):
        return (
            pltpu.make_async_copy(k_hbm.at[:, l], k.at[:, l, pl.ds(0, height)], load_sem.at[2, l]),
            pltpu.make_async_copy(act_hbm.at[l], act.at[l, pl.ds(0, height)], load_sem.at[3, l]),
            pltpu.make_async_copy(code_hbm.at[:, l], code.at[:, l], load_sem.at[4, l]),
            pltpu.make_async_copy(p_hbm.at[:, l], p.at[:, l, pl.ds(0, height)], load_sem.at[0, l]),
            pltpu.make_async_copy(a_hbm.at[:, l], a.at[:, l, pl.ds(0, height)], load_sem.at[1, l]),
        )

    def halo_pa(c):
        rows = pl.ds(c * ROWS, ROWS)
        return (
            pltpu.make_async_remote_copy(
                src_ref=p_hbm.at[:, 0, rows], dst_ref=halo_p.at[:, rows],
                send_sem=halo_send.at[2 * c], recv_sem=halo_recv.at[2 * c],
                device_id={"gx": lower}, device_id_type=MESH),
            pltpu.make_async_remote_copy(
                src_ref=a_hbm.at[:, 0, rows], dst_ref=halo_a.at[:, rows],
                send_sem=halo_send.at[2 * c + 1], recv_sem=halo_recv.at[2 * c + 1],
                device_id={"gx": lower}, device_id_type=MESH),
        )

    halo_k = pltpu.make_async_remote_copy(
        src_ref=g_out, dst_ref=halo_g, send_sem=halo_send.at[2 * blocks], recv_sem=halo_recv.at[2 * blocks],
        device_id={"gx": lower}, device_id_type=MESH)

    halo_first = pltpu.make_async_remote_copy(
        src_ref=grad.at[0, 0, pl.ds(height - ROWS, ROWS)], dst_ref=halo_own, send_sem=halo_send.at[2 * blocks + 1], recv_sem=halo_recv.at[2 * blocks + 1],
        device_id={"gx": lower}, device_id_type=MESH)

    def returned(c):
        rows = pl.ds(c * ROWS, ROWS)
        return pltpu.make_async_remote_copy(
            src_ref=ret_out.at[rows], dst_ref=ret_in.at[rows], send_sem=ret_send.at[c], recv_sem=ret_recv.at[c],
            device_id={"gx": upper}, device_id_type=MESH)

    first = loads(0)
    for copy in first[:3]:
        copy.start()

    await_signals(barrier, 1)

    @pl.when(me > 0)
    def _():
        for c in range(blocks // 2):
            for copy in halo_pa(c):
                copy.start()

    for copy in first[3:]:
        copy.start()

    def start_layer(l, carry):
        for copy in loads(l):
            copy.start()
        return carry

    lax.fori_loop(1, layers, start_layer, 0)
    for copy in first[:2]:
        copy.wait()
    g_out[...] = k[0, 0, 0:height] * act[0, 0:height].astype(jnp.float32)

    @pl.when(me > 0)
    def _():
        halo_k.start()

    for copy in first[2:]:
        copy.wait()
    tail[0:8] = jnp.zeros((8, width), jnp.float32)
    lane = lax.broadcasted_iota(jnp.int32, (ROWS, width), 1)
    row = lax.broadcasted_iota(jnp.int32, (ROWS, width), 0)
    grad[0, 0] = jnp.zeros((height, width), jnp.float32)

    def layer(l, total):
        @pl.when(l < last)
        def _():
            for copy in loads(l + 1):
                copy.wait()

        @pl.when(jnp.logical_and(l == 1, me > 0))
        def _():
            halo_first.start()
            for c in range(blocks // 2, blocks):
                for copy in halo_pa(c):
                    copy.start()

        def block(b, total):
            r = pl.multiple_of(b * ROWS, ROWS)
            here, after = pl.ds(r, ROWS), pl.ds(r + 1, ROWS)
            prod_y = jnp.zeros((ROWS, width), jnp.float32)
            prod_z = jnp.zeros((ROWS, width), jnp.float32)
            for t in range(steps):
                pt, at = p[t, l, here], a[t, l, here]
                prod_y += (at - a[t, l, after]) * (pt - p[t, l, after])
                prod_z += (at - pltpu.roll(at, width - 1, 1)) * (pt - pltpu.roll(pt, width - 1, 1))
            opened = act[l, here].astype(jnp.float32)
            k1 = k[1, l, here]
            k1_up = k[1, l, after]
            factor = multiplier(code[1, l, here]) * opened * act[l, after].astype(jnp.float32)
            w = jnp.where(row + r < height - 1, weight(prod_y, factor, k1, k1_up), 0.0)
            w_lo = jnp.where(row + r < height - 1, w * k1_up, 0.0)
            tail[pl.ds(r + 8, ROWS)] = w * k1
            log1 = w_lo + tail[pl.ds(r + 7, ROWS)]
            grad[1, l, here] = log1
            k2 = k[2, l, here]
            k2_up = pltpu.roll(k2, width - 1, 1)
            factor = multiplier(code[2, l, here]) * opened * pltpu.roll(opened, width - 1, 1)
            w = jnp.where(lane < width - 1, weight(prod_z, factor, k2, k2_up), 0.0)
            log2 = w * k2_up + pltpu.roll(w * k2, 1, 1)
            grad[2, l, here] = log2
            return total + fold(log1) + fold(log2)

        total = lax.fori_loop(0, blocks, block, total)

        def cross(b, total):
            here = pl.ds(pl.multiple_of(b * ROWS, ROWS), ROWS)
            prod = jnp.zeros((ROWS, width), jnp.float32)
            for t in range(steps):
                prod += (a[t, l, here] - a[t, l + 1, here]) * (p[t, l, here] - p[t, l + 1, here])
            k0, k0_up = k[0, l, here], k[0, l + 1, here]
            factor = multiplier(code[0, l, here]) * (act[l, here] * act[l + 1, here]).astype(jnp.float32)
            w = weight(prod, factor, k0, k0_up)
            log0 = grad[0, l, here] + w * k0_up
            grad[0, l, here] = log0
            grad[0, l + 1, here] = w * k0
            return total + jnp.where(l > 0, 1.0, 0.0) * fold(log0)

        return lax.cond(l < last, lambda total: lax.fori_loop(0, blocks, cross, total), lambda total: total, total)

    total = lax.fori_loop(0, layers, layer, jnp.zeros((8, width), jnp.float32))
    for i, distance in enumerate(distances(n)):
        signal(near_sem.at[i], distance)
        await_signals(near_sem.at[i], distance)

    acc[...] = total + jnp.where(me == 0, 1.0, 0.0) * fold(grad[0, 0])

    @pl.when(me < n - 1)
    def _():
        halo_k.wait_recv()
        for c in range(blocks):
            for copy in halo_pa(c):
                copy.wait_recv()
            here = pl.ds(c * ROWS, ROWS)
            prod = jnp.zeros((ROWS, width), jnp.float32)
            for t in range(steps):
                prod += (a[t, last, here] - halo_a[t, here]) * (p[t, last, here] - halo_p[t, here])
            k0, g_up = k[0, last, here], halo_g[here]
            factor = multiplier(code[0, last, here]) * act[last, here].astype(jnp.float32)
            w = weight(prod, factor, k0, g_up)
            w_up = w * k0
            ret_out[here] = w_up
            grad[0, last, here] = grad[0, last, here] + w * g_up
            if c < blocks - 1:
                returned(c).start()
            else:
                halo_first.wait_recv()
                acc[...] = acc[...] + fold(halo_own[...] + w_up)

    def take_back(c):
        here = pl.ds(c * ROWS, ROWS)
        returned(c).wait_recv()
        log0 = grad[0, 0, here] + ret_in[here]
        grad[0, 0, here] = log0
        return fold(log0)

    @pl.when(me > 0)
    def _():
        halo_first.wait_send()
        for c in range(blocks - 1):
            acc[...] = acc[...] + take_back(c)

    mine = jnp.sum(acc[...] + fold(grad[0, last]), axis=0, keepdims=True)
    part[...] = mine

    def to_peer(j):
        return pltpu.make_async_remote_copy(
            src_ref=part, dst_ref=parts.at[j - 1], send_sem=part_send.at[j - 1], recv_sem=part_recv.at[j - 1],
            device_id={"gx": lax.rem(me + j, n)}, device_id_type=MESH)

    def send(j, carry):
        to_peer(j).start()
        return carry

    def receive(j, carry):
        to_peer(j).wait_recv()
        return carry

    lax.fori_loop(1, n, send, 0)

    @pl.when(me < n - 1)
    def _():
        returned(blocks - 1).start()

    @pl.when(me > 0)
    def _():
        take_back(blocks - 1)

    lax.fori_loop(1, n, receive, 0)
    whole = jnp.sum(jnp.sum(parts[...], axis=0) + mine, keepdims=True)
    scale = jnp.broadcast_to(lax.rsqrt(whole / entries + epsilon), (ROWS, width))

    def normalize(i, carry):
        here = pl.ds(pl.multiple_of(i * ROWS, ROWS), ROWS)
        for d in range(3):
            for l in range(layers):
                grad[d, l, here] = grad[d, l, here] * scale
        return carry

    lax.fori_loop(0, blocks, normalize, 0)

    def drain(j, carry):
        to_peer(j).wait_send()
        return carry

    lax.fori_loop(1, n, drain, 0)

    @pl.when(me > 0)
    def _():
        halo_k.wait_send()
        for c in range(blocks):
            for copy in halo_pa(c):
                copy.wait_send()

    @pl.when(me < n - 1)
    def _():
        for c in range(blocks):
            returned(c).wait_send()


def local(pressure, adjoint, permeability, active, fault_codes):
    n = lax.axis_size("gx")
    steps, layers, height, width = pressure.shape
    blocks = height // ROWS
    entries = 3 * layers * n * height * width
    f32 = jnp.float32
    padded = height + PAD
    dma = pltpu.SemaphoreType.DMA
    return pl.pallas_call(
        functools.partial(kernel, n, entries),
        out_shape=pltpu.VMEM((3, layers, height, width), f32),
        in_specs=[pl.BlockSpec(memory_space=pltpu.HBM)] * 5,
        out_specs=pl.BlockSpec(memory_space=pltpu.VMEM),
        scratch_shapes=[
            pltpu.VMEM((steps, layers, padded, width), f32),
            pltpu.VMEM((steps, layers, padded, width), f32),
            pltpu.VMEM((3, layers, padded, width), f32),
            pltpu.VMEM((layers, padded, width), jnp.int32),
            pltpu.VMEM((3, layers, height, width), jnp.int32),
            pltpu.VMEM((steps, height, width), f32),
            pltpu.VMEM((steps, height, width), f32),
            pltpu.VMEM((height, width), f32),
            pltpu.VMEM((ROWS, width), f32),
            pltpu.VMEM((height, width), f32),
            pltpu.VMEM((height, width), f32),
            pltpu.VMEM((height, width), f32),
            pltpu.VMEM((padded, width), f32),
            pltpu.VMEM((8, width), f32),
            pltpu.VMEM((1, width), f32),
            pltpu.VMEM((n - 1, 1, width), f32),
            dma((5, layers)),
            dma((2 * blocks + 2,)),
            dma((2 * blocks + 2,)),
            dma((blocks,)),
            dma((blocks,)),
            dma((n - 1,)),
            dma((n - 1,)),
            pltpu.SemaphoreType.REGULAR((len(distances(n)),)),
        ],
        compiler_params=pltpu.CompilerParams(collective_id=0, has_side_effects=True, vmem_limit_bytes=GRANT),
        cost_estimate=pl.CostEstimate(flops=100_000_000, bytes_accessed=12_000_000, transcendentals=0),
    )(pressure, adjoint, permeability, active, fault_codes)


def solution(mesh):
    split = ("groups", "gx")
    placed = (P(None, split), P(None, split), P(None, split), P(split), P(None, split))
    return jax.shard_map(local, mesh=mesh, in_specs=placed, out_specs=P(None, split), check_vma=False)
```

```python
import functools

import jax
import jax.numpy as jnp
from jax import lax
from jax.experimental import pallas as pl
from jax.experimental.pallas import tpu as pltpu
from jax.sharding import PartitionSpec as P

MESH = pl.DeviceIdType.MESH
epsilon = 1e-06
ROWS = 32
PAD = 8
GRANT = 58_000_000


def multiplier(codes):
    return jnp.where(codes == 0, 1.0, jnp.where(codes == 1, 0.6, jnp.where(codes == 2, 0.25, 0.05))).astype(jnp.float32)


def fold(values):
    squares = values * values
    total = squares[0:8]
    for i in range(8, squares.shape[0], 8):
        total = total + squares[i : i + 8]
    return total


def weight(products, factor, k_lo, k_up):
    summed = k_lo + k_up
    return 2.0 * factor * products * (k_lo * k_up) / (summed * summed)


def kernel(
    n, entries, p_hbm, a_hbm, k_hbm, act_hbm, code_hbm, grad,
    p, a, k, act, code, halo_p, halo_a, halo_g, halo_own, g_out, ret_out, ret_in, tail, acc, part, parts,
    load_sem, halo_send, halo_recv, ret_send, ret_recv, part_send, part_recv,
):
    me = lax.axis_index("gx")
    lower, upper = me - 1, me + 1
    steps, layers, height, width = p_hbm.shape
    last = layers - 1
    blocks = height // ROWS

    barrier = pltpu.get_barrier_semaphore()

    def greet(j, carry):
        pl.semaphore_signal(barrier, inc=1, device_id={"gx": lax.rem(me + j, n)}, device_id_type=MESH)
        return carry

    lax.fori_loop(1, n, greet, 0)

    def loads(l):
        return (
            pltpu.make_async_copy(k_hbm.at[:, l], k.at[:, l, pl.ds(0, height)], load_sem.at[2, l]),
            pltpu.make_async_copy(act_hbm.at[l], act.at[l, pl.ds(0, height)], load_sem.at[3, l]),
            pltpu.make_async_copy(code_hbm.at[:, l], code.at[:, l], load_sem.at[4, l]),
            pltpu.make_async_copy(p_hbm.at[:, l], p.at[:, l, pl.ds(0, height)], load_sem.at[0, l]),
            pltpu.make_async_copy(a_hbm.at[:, l], a.at[:, l, pl.ds(0, height)], load_sem.at[1, l]),
        )

    def halo_pa(c):
        rows = pl.ds(c * ROWS, ROWS)
        return (
            pltpu.make_async_remote_copy(
                src_ref=p_hbm.at[:, 0, rows], dst_ref=halo_p.at[:, rows],
                send_sem=halo_send.at[2 * c], recv_sem=halo_recv.at[2 * c],
                device_id={"gx": lower}, device_id_type=MESH),
            pltpu.make_async_remote_copy(
                src_ref=a_hbm.at[:, 0, rows], dst_ref=halo_a.at[:, rows],
                send_sem=halo_send.at[2 * c + 1], recv_sem=halo_recv.at[2 * c + 1],
                device_id={"gx": lower}, device_id_type=MESH),
        )

    halo_k = pltpu.make_async_remote_copy(
        src_ref=g_out, dst_ref=halo_g, send_sem=halo_send.at[2 * blocks], recv_sem=halo_recv.at[2 * blocks],
        device_id={"gx": lower}, device_id_type=MESH)

    halo_first = pltpu.make_async_remote_copy(
        src_ref=grad.at[0, 0, pl.ds(height - ROWS, ROWS)], dst_ref=halo_own, send_sem=halo_send.at[2 * blocks + 1], recv_sem=halo_recv.at[2 * blocks + 1],
        device_id={"gx": lower}, device_id_type=MESH)

    def returned(c):
        rows = pl.ds(c * ROWS, ROWS)
        return pltpu.make_async_remote_copy(
            src_ref=ret_out.at[rows], dst_ref=ret_in.at[rows], send_sem=ret_send.at[c], recv_sem=ret_recv.at[c],
            device_id={"gx": upper}, device_id_type=MESH)

    first = loads(0)
    for copy in first[:3]:
        copy.start()

    pl.semaphore_wait(barrier, n - 1)

    @pl.when(me > 0)
    def _():
        for c in range(blocks // 2):
            for copy in halo_pa(c):
                copy.start()

    for copy in first[3:]:
        copy.start()

    def start_layer(l, carry):
        for copy in loads(l):
            copy.start()
        return carry

    lax.fori_loop(1, layers, start_layer, 0)
    for copy in first[:2]:
        copy.wait()
    g_out[...] = k[0, 0, 0:height] * act[0, 0:height].astype(jnp.float32)

    @pl.when(me > 0)
    def _():
        halo_k.start()

    for copy in first[2:]:
        copy.wait()
    tail[0:8] = jnp.zeros((8, width), jnp.float32)
    lane = lax.broadcasted_iota(jnp.int32, (ROWS, width), 1)
    row = lax.broadcasted_iota(jnp.int32, (ROWS, width), 0)
    grad[0, 0] = jnp.zeros((height, width), jnp.float32)

    def layer(l, total):
        @pl.when(l < last)
        def _():
            for copy in loads(l + 1):
                copy.wait()

        @pl.when(jnp.logical_and(l == 1, me > 0))
        def _():
            halo_first.start()
            for c in range(blocks // 2, blocks):
                for copy in halo_pa(c):
                    copy.start()

        def block(b, total):
            r = pl.multiple_of(b * ROWS, ROWS)
            here, after = pl.ds(r, ROWS), pl.ds(r + 1, ROWS)
            prod_y = jnp.zeros((ROWS, width), jnp.float32)
            prod_z = jnp.zeros((ROWS, width), jnp.float32)
            for t in range(steps):
                pt, at = p[t, l, here], a[t, l, here]
                prod_y += (at - a[t, l, after]) * (pt - p[t, l, after])
                prod_z += (at - pltpu.roll(at, width - 1, 1)) * (pt - pltpu.roll(pt, width - 1, 1))
            opened = act[l, here].astype(jnp.float32)
            k1 = k[1, l, here]
            k1_up = k[1, l, after]
            factor = multiplier(code[1, l, here]) * opened * act[l, after].astype(jnp.float32)
            w = jnp.where(row + r < height - 1, weight(prod_y, factor, k1, k1_up), 0.0)
            w_lo = jnp.where(row + r < height - 1, w * k1_up, 0.0)
            tail[pl.ds(r + 8, ROWS)] = w * k1
            log1 = w_lo + tail[pl.ds(r + 7, ROWS)]
            grad[1, l, here] = log1
            k2 = k[2, l, here]
            k2_up = pltpu.roll(k2, width - 1, 1)
            factor = multiplier(code[2, l, here]) * opened * pltpu.roll(opened, width - 1, 1)
            w = jnp.where(lane < width - 1, weight(prod_z, factor, k2, k2_up), 0.0)
            log2 = w * k2_up + pltpu.roll(w * k2, 1, 1)
            grad[2, l, here] = log2
            return total + fold(log1) + fold(log2)

        total = lax.fori_loop(0, blocks, block, total)

        def cross(b, total):
            here = pl.ds(pl.multiple_of(b * ROWS, ROWS), ROWS)
            prod = jnp.zeros((ROWS, width), jnp.float32)
            for t in range(steps):
                prod += (a[t, l, here] - a[t, l + 1, here]) * (p[t, l, here] - p[t, l + 1, here])
            k0, k0_up = k[0, l, here], k[0, l + 1, here]
            factor = multiplier(code[0, l, here]) * (act[l, here] * act[l + 1, here]).astype(jnp.float32)
            w = weight(prod, factor, k0, k0_up)
            log0 = grad[0, l, here] + w * k0_up
            grad[0, l, here] = log0
            grad[0, l + 1, here] = w * k0
            return total + jnp.where(l > 0, 1.0, 0.0) * fold(log0)

        return lax.cond(l < last, lambda total: lax.fori_loop(0, blocks, cross, total), lambda total: total, total)

    total = lax.fori_loop(0, layers, layer, jnp.zeros((8, width), jnp.float32))
    acc[...] = total + jnp.where(me == 0, 1.0, 0.0) * fold(grad[0, 0])

    @pl.when(me < n - 1)
    def _():
        halo_k.wait_recv()
        for c in range(blocks):
            for copy in halo_pa(c):
                copy.wait_recv()
            here = pl.ds(c * ROWS, ROWS)
            prod = jnp.zeros((ROWS, width), jnp.float32)
            for t in range(steps):
                prod += (a[t, last, here] - halo_a[t, here]) * (p[t, last, here] - halo_p[t, here])
            k0, g_up = k[0, last, here], halo_g[here]
            factor = multiplier(code[0, last, here]) * act[last, here].astype(jnp.float32)
            w = weight(prod, factor, k0, g_up)
            w_up = w * k0
            ret_out[here] = w_up
            grad[0, last, here] = grad[0, last, here] + w * g_up
            if c < blocks - 1:
                returned(c).start()
            else:
                halo_first.wait_recv()
                acc[...] = acc[...] + fold(halo_own[...] + w_up)

    def take_back(c):
        here = pl.ds(c * ROWS, ROWS)
        returned(c).wait_recv()
        log0 = grad[0, 0, here] + ret_in[here]
        grad[0, 0, here] = log0
        return fold(log0)

    @pl.when(me > 0)
    def _():
        halo_first.wait_send()
        for c in range(blocks - 1):
            acc[...] = acc[...] + take_back(c)

    mine = jnp.sum(acc[...] + fold(grad[0, last]), axis=0, keepdims=True)
    part[...] = mine

    def to_peer(j):
        return pltpu.make_async_remote_copy(
            src_ref=part, dst_ref=parts.at[j - 1], send_sem=part_send.at[j - 1], recv_sem=part_recv.at[j - 1],
            device_id={"gx": lax.rem(me + j, n)}, device_id_type=MESH)

    def send(j, carry):
        to_peer(j).start()
        return carry

    def receive(j, carry):
        to_peer(j).wait_recv()
        return carry

    lax.fori_loop(1, n, send, 0)

    @pl.when(me < n - 1)
    def _():
        returned(blocks - 1).start()

    @pl.when(me > 0)
    def _():
        take_back(blocks - 1)

    lax.fori_loop(1, n, receive, 0)
    whole = jnp.sum(jnp.sum(parts[...], axis=0) + mine, keepdims=True)
    scale = jnp.broadcast_to(lax.rsqrt(whole / entries + epsilon), (ROWS, width))

    def normalize(i, carry):
        here = pl.ds(pl.multiple_of(i * ROWS, ROWS), ROWS)
        for d in range(3):
            for l in range(layers):
                grad[d, l, here] = grad[d, l, here] * scale
        return carry

    lax.fori_loop(0, blocks, normalize, 0)

    def drain(j, carry):
        to_peer(j).wait_send()
        return carry

    lax.fori_loop(1, n, drain, 0)

    @pl.when(me > 0)
    def _():
        halo_k.wait_send()
        for c in range(blocks):
            for copy in halo_pa(c):
                copy.wait_send()

    @pl.when(me < n - 1)
    def _():
        for c in range(blocks):
            returned(c).wait_send()


def local(pressure, adjoint, permeability, active, fault_codes):
    n = lax.axis_size("gx")
    steps, layers, height, width = pressure.shape
    blocks = height // ROWS
    entries = 3 * layers * n * height * width
    f32 = jnp.float32
    padded = height + PAD
    dma = pltpu.SemaphoreType.DMA
    return pl.pallas_call(
        functools.partial(kernel, n, entries),
        out_shape=pltpu.VMEM((3, layers, height, width), f32),
        in_specs=[pl.BlockSpec(memory_space=pltpu.HBM)] * 5,
        out_specs=pl.BlockSpec(memory_space=pltpu.VMEM),
        scratch_shapes=[
            pltpu.VMEM((steps, layers, padded, width), f32),
            pltpu.VMEM((steps, layers, padded, width), f32),
            pltpu.VMEM((3, layers, padded, width), f32),
            pltpu.VMEM((layers, padded, width), jnp.int32),
            pltpu.VMEM((3, layers, height, width), jnp.int32),
            pltpu.VMEM((steps, height, width), f32),
            pltpu.VMEM((steps, height, width), f32),
            pltpu.VMEM((height, width), f32),
            pltpu.VMEM((ROWS, width), f32),
            pltpu.VMEM((height, width), f32),
            pltpu.VMEM((height, width), f32),
            pltpu.VMEM((height, width), f32),
            pltpu.VMEM((padded, width), f32),
            pltpu.VMEM((8, width), f32),
            pltpu.VMEM((1, width), f32),
            pltpu.VMEM((n - 1, 1, width), f32),
            dma((5, layers)),
            dma((2 * blocks + 2,)),
            dma((2 * blocks + 2,)),
            dma((blocks,)),
            dma((blocks,)),
            dma((n - 1,)),
            dma((n - 1,)),
        ],
        compiler_params=pltpu.CompilerParams(collective_id=0, has_side_effects=True, vmem_limit_bytes=GRANT),
        cost_estimate=pl.CostEstimate(flops=100_000_000, bytes_accessed=12_000_000, transcendentals=0),
    )(pressure, adjoint, permeability, active, fault_codes)


def solution(mesh):
    split = ("groups", "gx")
    placed = (P(None, split), P(None, split), P(None, split), P(split), P(None, split))
    return jax.shard_map(local, mesh=mesh, in_specs=placed, out_specs=P(None, split), check_vma=False)
```

```python
import functools

import jax
import jax.numpy as jnp
from jax import lax
from jax.experimental import pallas as pl
from jax.experimental.pallas import tpu as pltpu
from jax.sharding import PartitionSpec as P

MESH = pl.DeviceIdType.MESH
epsilon = 1e-06
ROWS = 32
PAD = 8
GRANT = 58_000_000


def multiplier(codes):
    return jnp.where(codes == 0, 1.0, jnp.where(codes == 1, 0.6, jnp.where(codes == 2, 0.25, 0.05))).astype(jnp.float32)


def fold(values):
    squares = values * values
    total = squares[0:8]
    for i in range(8, squares.shape[0], 8):
        total = total + squares[i : i + 8]
    return total


def weight(products, factor, k_lo, k_up):
    summed = k_lo + k_up
    return 2.0 * factor * products * (k_lo * k_up) / (summed * summed)


def distances(n):
    reach, rounds = 1, []
    while reach < n - 1:
        rounds.append(reach)
        reach *= 2
    return rounds


def kernel(
    n, entries, p_hbm, a_hbm, k_hbm, act_hbm, code_hbm, grad,
    p, a, k, act, code, halo_p, halo_a, halo_g, halo_own, g_out, ret_out, ret_in, tail, acc, part, parts,
    load_sem, halo_send, halo_recv, ret_send, ret_recv, part_send, part_recv, near_sem,
):
    me = lax.axis_index("gx")
    lower, upper = me - 1, me + 1
    steps, layers, height, width = p_hbm.shape
    last = layers - 1
    blocks = height // ROWS

    barrier = pltpu.get_barrier_semaphore()

    def signal(semaphore, distance):
        for there, inside in ((me - distance, me >= distance), (me + distance, me + distance < n)):
            @pl.when(inside)
            def _():
                pl.semaphore_signal(semaphore, inc=1, device_id={"gx": there}, device_id_type=MESH)

    def await_signals(semaphore, distance):
        peers = jnp.where(me >= distance, 1, 0) + jnp.where(me + distance < n, 1, 0)
        pl.semaphore_wait(semaphore, peers)

    signal(barrier, 1)
    rounds = distances(n)

    def turn(i):
        if i > 0:
            await_signals(near_sem.at[i - 1], rounds[i - 1])
        if i < len(rounds):
            signal(near_sem.at[i], rounds[i])

    def loads(l):
        return (
            pltpu.make_async_copy(k_hbm.at[:, l], k.at[:, l, pl.ds(0, height)], load_sem.at[2, l]),
            pltpu.make_async_copy(act_hbm.at[l], act.at[l, pl.ds(0, height)], load_sem.at[3, l]),
            pltpu.make_async_copy(code_hbm.at[:, l], code.at[:, l], load_sem.at[4, l]),
            pltpu.make_async_copy(p_hbm.at[:, l], p.at[:, l, pl.ds(0, height)], load_sem.at[0, l]),
            pltpu.make_async_copy(a_hbm.at[:, l], a.at[:, l, pl.ds(0, height)], load_sem.at[1, l]),
        )

    def halo_pa(c):
        rows = pl.ds(c * ROWS, ROWS)
        return (
            pltpu.make_async_remote_copy(
                src_ref=p_hbm.at[:, 0, rows], dst_ref=halo_p.at[:, rows],
                send_sem=halo_send.at[2 * c], recv_sem=halo_recv.at[2 * c],
                device_id={"gx": lower}, device_id_type=MESH),
            pltpu.make_async_remote_copy(
                src_ref=a_hbm.at[:, 0, rows], dst_ref=halo_a.at[:, rows],
                send_sem=halo_send.at[2 * c + 1], recv_sem=halo_recv.at[2 * c + 1],
                device_id={"gx": lower}, device_id_type=MESH),
        )

    halo_k = pltpu.make_async_remote_copy(
        src_ref=g_out, dst_ref=halo_g, send_sem=halo_send.at[2 * blocks], recv_sem=halo_recv.at[2 * blocks],
        device_id={"gx": lower}, device_id_type=MESH)

    halo_first = pltpu.make_async_remote_copy(
        src_ref=grad.at[0, 0, pl.ds(height - ROWS, ROWS)], dst_ref=halo_own, send_sem=halo_send.at[2 * blocks + 1], recv_sem=halo_recv.at[2 * blocks + 1],
        device_id={"gx": lower}, device_id_type=MESH)

    def returned(c):
        rows = pl.ds(c * ROWS, ROWS)
        return pltpu.make_async_remote_copy(
            src_ref=ret_out.at[rows], dst_ref=ret_in.at[rows], send_sem=ret_send.at[c], recv_sem=ret_recv.at[c],
            device_id={"gx": upper}, device_id_type=MESH)

    first = loads(0)
    for copy in first[:3]:
        copy.start()

    await_signals(barrier, 1)
    turn(0)

    @pl.when(me > 0)
    def _():
        for c in range(blocks // 2):
            for copy in halo_pa(c):
                copy.start()

    for copy in first[3:]:
        copy.start()

    def start_layer(l, carry):
        for copy in loads(l):
            copy.start()
        return carry

    lax.fori_loop(1, layers, start_layer, 0)
    for copy in first[:2]:
        copy.wait()
    g_out[...] = k[0, 0, 0:height] * act[0, 0:height].astype(jnp.float32)

    @pl.when(me > 0)
    def _():
        halo_k.start()

    for copy in first[2:]:
        copy.wait()
    tail[0:8] = jnp.zeros((8, width), jnp.float32)
    lane = lax.broadcasted_iota(jnp.int32, (ROWS, width), 1)
    row = lax.broadcasted_iota(jnp.int32, (ROWS, width), 0)
    grad[0, 0] = jnp.zeros((height, width), jnp.float32)

    def layer(l, total):
        @pl.when(l < last)
        def _():
            for copy in loads(l + 1):
                copy.wait()

        @pl.when(jnp.logical_and(l == 1, me > 0))
        def _():
            halo_first.start()
            for c in range(blocks // 2, blocks):
                for copy in halo_pa(c):
                    copy.start()

        for i in range(1, min(layers - 1, len(rounds) + 1)):
            @pl.when(l == i + 1)
            def _(i=i):
                turn(i)

        def block(b, total):
            r = pl.multiple_of(b * ROWS, ROWS)
            here, after = pl.ds(r, ROWS), pl.ds(r + 1, ROWS)
            prod_y = jnp.zeros((ROWS, width), jnp.float32)
            prod_z = jnp.zeros((ROWS, width), jnp.float32)
            for t in range(steps):
                pt, at = p[t, l, here], a[t, l, here]
                prod_y += (at - a[t, l, after]) * (pt - p[t, l, after])
                prod_z += (at - pltpu.roll(at, width - 1, 1)) * (pt - pltpu.roll(pt, width - 1, 1))
            opened = act[l, here].astype(jnp.float32)
            k1 = k[1, l, here]
            k1_up = k[1, l, after]
            factor = multiplier(code[1, l, here]) * opened * act[l, after].astype(jnp.float32)
            w = jnp.where(row + r < height - 1, weight(prod_y, factor, k1, k1_up), 0.0)
            w_lo = jnp.where(row + r < height - 1, w * k1_up, 0.0)
            tail[pl.ds(r + 8, ROWS)] = w * k1
            log1 = w_lo + tail[pl.ds(r + 7, ROWS)]
            grad[1, l, here] = log1
            k2 = k[2, l, here]
            k2_up = pltpu.roll(k2, width - 1, 1)
            factor = multiplier(code[2, l, here]) * opened * pltpu.roll(opened, width - 1, 1)
            w = jnp.where(lane < width - 1, weight(prod_z, factor, k2, k2_up), 0.0)
            log2 = w * k2_up + pltpu.roll(w * k2, 1, 1)
            grad[2, l, here] = log2
            return total + fold(log1) + fold(log2)

        total = lax.fori_loop(0, blocks, block, total)

        def cross(b, total):
            here = pl.ds(pl.multiple_of(b * ROWS, ROWS), ROWS)
            prod = jnp.zeros((ROWS, width), jnp.float32)
            for t in range(steps):
                prod += (a[t, l, here] - a[t, l + 1, here]) * (p[t, l, here] - p[t, l + 1, here])
            k0, k0_up = k[0, l, here], k[0, l + 1, here]
            factor = multiplier(code[0, l, here]) * (act[l, here] * act[l + 1, here]).astype(jnp.float32)
            w = weight(prod, factor, k0, k0_up)
            log0 = grad[0, l, here] + w * k0_up
            grad[0, l, here] = log0
            grad[0, l + 1, here] = w * k0
            return total + jnp.where(l > 0, 1.0, 0.0) * fold(log0)

        return lax.cond(l < last, lambda total: lax.fori_loop(0, blocks, cross, total), lambda total: total, total)

    total = lax.fori_loop(0, layers, layer, jnp.zeros((8, width), jnp.float32))
    for i in range(layers - 1, len(rounds) + 1):
        turn(i)

    acc[...] = total + jnp.where(me == 0, 1.0, 0.0) * fold(grad[0, 0])

    @pl.when(me < n - 1)
    def _():
        halo_k.wait_recv()
        for c in range(blocks):
            for copy in halo_pa(c):
                copy.wait_recv()
            here = pl.ds(c * ROWS, ROWS)
            prod = jnp.zeros((ROWS, width), jnp.float32)
            for t in range(steps):
                prod += (a[t, last, here] - halo_a[t, here]) * (p[t, last, here] - halo_p[t, here])
            k0, g_up = k[0, last, here], halo_g[here]
            factor = multiplier(code[0, last, here]) * act[last, here].astype(jnp.float32)
            w = weight(prod, factor, k0, g_up)
            w_up = w * k0
            ret_out[here] = w_up
            grad[0, last, here] = grad[0, last, here] + w * g_up
            if c < blocks - 1:
                returned(c).start()
            else:
                halo_first.wait_recv()
                acc[...] = acc[...] + fold(halo_own[...] + w_up)

    def take_back(c):
        here = pl.ds(c * ROWS, ROWS)
        returned(c).wait_recv()
        log0 = grad[0, 0, here] + ret_in[here]
        grad[0, 0, here] = log0
        return fold(log0)

    @pl.when(me > 0)
    def _():
        halo_first.wait_send()
        for c in range(blocks - 1):
            acc[...] = acc[...] + take_back(c)

    mine = jnp.sum(acc[...] + fold(grad[0, last]), axis=0, keepdims=True)
    part[...] = mine

    def to_peer(j):
        return pltpu.make_async_remote_copy(
            src_ref=part, dst_ref=parts.at[j - 1], send_sem=part_send.at[j - 1], recv_sem=part_recv.at[j - 1],
            device_id={"gx": lax.rem(me + j, n)}, device_id_type=MESH)

    def send(j, carry):
        to_peer(j).start()
        return carry

    def receive(j, carry):
        to_peer(j).wait_recv()
        return carry

    lax.fori_loop(1, n, send, 0)

    @pl.when(me < n - 1)
    def _():
        returned(blocks - 1).start()

    @pl.when(me > 0)
    def _():
        take_back(blocks - 1)

    lax.fori_loop(1, n, receive, 0)
    whole = jnp.sum(jnp.sum(parts[...], axis=0) + mine, keepdims=True)
    scale = jnp.broadcast_to(lax.rsqrt(whole / entries + epsilon), (ROWS, width))

    def normalize(i, carry):
        here = pl.ds(pl.multiple_of(i * ROWS, ROWS), ROWS)
        for d in range(3):
            for l in range(layers):
                grad[d, l, here] = grad[d, l, here] * scale
        return carry

    lax.fori_loop(0, blocks, normalize, 0)

    def drain(j, carry):
        to_peer(j).wait_send()
        return carry

    lax.fori_loop(1, n, drain, 0)

    @pl.when(me > 0)
    def _():
        halo_k.wait_send()
        for c in range(blocks):
            for copy in halo_pa(c):
                copy.wait_send()

    @pl.when(me < n - 1)
    def _():
        for c in range(blocks):
            returned(c).wait_send()


def local(pressure, adjoint, permeability, active, fault_codes):
    n = lax.axis_size("gx")
    steps, layers, height, width = pressure.shape
    blocks = height // ROWS
    entries = 3 * layers * n * height * width
    f32 = jnp.float32
    padded = height + PAD
    dma = pltpu.SemaphoreType.DMA
    return pl.pallas_call(
        functools.partial(kernel, n, entries),
        out_shape=pltpu.VMEM((3, layers, height, width), f32),
        in_specs=[pl.BlockSpec(memory_space=pltpu.HBM)] * 5,
        out_specs=pl.BlockSpec(memory_space=pltpu.VMEM),
        scratch_shapes=[
            pltpu.VMEM((steps, layers, padded, width), f32),
            pltpu.VMEM((steps, layers, padded, width), f32),
            pltpu.VMEM((3, layers, padded, width), f32),
            pltpu.VMEM((layers, padded, width), jnp.int32),
            pltpu.VMEM((3, layers, height, width), jnp.int32),
            pltpu.VMEM((steps, height, width), f32),
            pltpu.VMEM((steps, height, width), f32),
            pltpu.VMEM((height, width), f32),
            pltpu.VMEM((ROWS, width), f32),
            pltpu.VMEM((height, width), f32),
            pltpu.VMEM((height, width), f32),
            pltpu.VMEM((height, width), f32),
            pltpu.VMEM((padded, width), f32),
            pltpu.VMEM((8, width), f32),
            pltpu.VMEM((1, width), f32),
            pltpu.VMEM((n - 1, 1, width), f32),
            dma((5, layers)),
            dma((2 * blocks + 2,)),
            dma((2 * blocks + 2,)),
            dma((blocks,)),
            dma((blocks,)),
            dma((n - 1,)),
            dma((n - 1,)),
            pltpu.SemaphoreType.REGULAR((len(distances(n)),)),
        ],
        compiler_params=pltpu.CompilerParams(collective_id=0, has_side_effects=True, vmem_limit_bytes=GRANT),
        cost_estimate=pl.CostEstimate(flops=100_000_000, bytes_accessed=12_000_000, transcendentals=0),
    )(pressure, adjoint, permeability, active, fault_codes)


def solution(mesh):
    split = ("groups", "gx")
    placed = (P(None, split), P(None, split), P(None, split), P(split), P(None, split))
    return jax.shard_map(local, mesh=mesh, in_specs=placed, out_specs=P(None, split), check_vma=False)
```

```python
import functools

import jax
import jax.numpy as jnp
from jax import lax
from jax.experimental import pallas as pl
from jax.experimental.pallas import tpu as pltpu
from jax.sharding import PartitionSpec as P

MESH = pl.DeviceIdType.MESH
epsilon = 1e-06
ROWS = 32
PAD = 8
GRANT = 58_000_000


def multiplier(codes):
    return jnp.where(codes == 0, 1.0, jnp.where(codes == 1, 0.6, jnp.where(codes == 2, 0.25, 0.05))).astype(jnp.float32)


def fold(values):
    squares = values * values
    total = squares[0:8]
    for i in range(8, squares.shape[0], 8):
        total = total + squares[i : i + 8]
    return total


def weight(products, factor, k_lo, k_up):
    summed = k_lo + k_up
    return 2.0 * factor * products * (k_lo * k_up) / (summed * summed)


def distances(n):
    reach, rounds = 1, []
    while reach < n - 1:
        rounds.append(reach)
        reach *= 2
    return rounds


def kernel(
    n, entries, p_hbm, a_hbm, k_hbm, act_hbm, code_hbm, grad,
    p, a, k, act, code, halo_p, halo_a, halo_g, halo_own, g_out, ret_out, ret_in, tail, acc, part, parts,
    load_sem, halo_send, halo_recv, ret_send, ret_recv, part_send, part_recv, near_sem,
):
    me = lax.axis_index("gx")
    lower, upper = me - 1, me + 1
    steps, layers, height, width = p_hbm.shape
    last = layers - 1
    blocks = height // ROWS

    barrier = pltpu.get_barrier_semaphore()

    def signal(semaphore, distance):
        for there, inside in ((me - distance, me >= distance), (me + distance, me + distance < n)):
            @pl.when(inside)
            def _():
                pl.semaphore_signal(semaphore, inc=1, device_id={"gx": there}, device_id_type=MESH)

    def await_signals(semaphore, distance):
        peers = jnp.where(me >= distance, 1, 0) + jnp.where(me + distance < n, 1, 0)
        pl.semaphore_wait(semaphore, peers)

    @pl.when(upper < n)
    def _():
        pl.semaphore_signal(barrier, inc=1, device_id={"gx": upper}, device_id_type=MESH)

    rounds = distances(n)

    def turn(i):
        if i > 0:
            await_signals(near_sem.at[i - 1], rounds[i - 1])
        else:
            @pl.when(upper < n)
            def _():
                pl.semaphore_wait(near_sem.at[len(rounds)], 1)

        if i < len(rounds):
            signal(near_sem.at[i], rounds[i])

    def loads(l):
        return (
            pltpu.make_async_copy(k_hbm.at[:, l], k.at[:, l, pl.ds(0, height)], load_sem.at[2, l]),
            pltpu.make_async_copy(act_hbm.at[l], act.at[l, pl.ds(0, height)], load_sem.at[3, l]),
            pltpu.make_async_copy(code_hbm.at[:, l], code.at[:, l], load_sem.at[4, l]),
            pltpu.make_async_copy(p_hbm.at[:, l], p.at[:, l, pl.ds(0, height)], load_sem.at[0, l]),
            pltpu.make_async_copy(a_hbm.at[:, l], a.at[:, l, pl.ds(0, height)], load_sem.at[1, l]),
        )

    def halo_pa(c):
        rows = pl.ds(c * ROWS, ROWS)
        return (
            pltpu.make_async_remote_copy(
                src_ref=p_hbm.at[:, 0, rows], dst_ref=halo_p.at[:, rows],
                send_sem=halo_send.at[2 * c], recv_sem=halo_recv.at[2 * c],
                device_id={"gx": lower}, device_id_type=MESH),
            pltpu.make_async_remote_copy(
                src_ref=a_hbm.at[:, 0, rows], dst_ref=halo_a.at[:, rows],
                send_sem=halo_send.at[2 * c + 1], recv_sem=halo_recv.at[2 * c + 1],
                device_id={"gx": lower}, device_id_type=MESH),
        )

    halo_k = pltpu.make_async_remote_copy(
        src_ref=g_out, dst_ref=halo_g, send_sem=halo_send.at[2 * blocks], recv_sem=halo_recv.at[2 * blocks],
        device_id={"gx": lower}, device_id_type=MESH)

    halo_first = pltpu.make_async_remote_copy(
        src_ref=grad.at[0, 0, pl.ds(height - ROWS, ROWS)], dst_ref=halo_own, send_sem=halo_send.at[2 * blocks + 1], recv_sem=halo_recv.at[2 * blocks + 1],
        device_id={"gx": lower}, device_id_type=MESH)

    def returned(c):
        rows = pl.ds(c * ROWS, ROWS)
        return pltpu.make_async_remote_copy(
            src_ref=ret_out.at[rows], dst_ref=ret_in.at[rows], send_sem=ret_send.at[c], recv_sem=ret_recv.at[c],
            device_id={"gx": upper}, device_id_type=MESH)

    first = loads(0)
    for copy in first[:3]:
        copy.start()

    @pl.when(me > 0)
    def _():
        pl.semaphore_wait(barrier, 1)
        pl.semaphore_signal(near_sem.at[len(rounds)], inc=1, device_id={"gx": lower}, device_id_type=MESH)


    @pl.when(me > 0)
    def _():
        for c in range(blocks // 2):
            for copy in halo_pa(c):
                copy.start()

    for copy in first[3:]:
        copy.start()

    def start_layer(l, carry):
        for copy in loads(l):
            copy.start()
        return carry

    lax.fori_loop(1, layers, start_layer, 0)
    for copy in first[:2]:
        copy.wait()
    g_out[...] = k[0, 0, 0:height] * act[0, 0:height].astype(jnp.float32)

    @pl.when(me > 0)
    def _():
        halo_k.start()

    for copy in first[2:]:
        copy.wait()
    tail[0:8] = jnp.zeros((8, width), jnp.float32)
    lane = lax.broadcasted_iota(jnp.int32, (ROWS, width), 1)
    row = lax.broadcasted_iota(jnp.int32, (ROWS, width), 0)
    grad[0, 0] = jnp.zeros((height, width), jnp.float32)

    def layer(l, total):
        @pl.when(l < last)
        def _():
            for copy in loads(l + 1):
                copy.wait()

        @pl.when(jnp.logical_and(l == 1, me > 0))
        def _():
            halo_first.start()
            for c in range(blocks // 2, blocks):
                for copy in halo_pa(c):
                    copy.start()

        for i in range(0, min(layers - 1, len(rounds) + 1)):
            @pl.when(l == i + 1)
            def _(i=i):
                turn(i)

        def block(b, total):
            r = pl.multiple_of(b * ROWS, ROWS)
            here, after = pl.ds(r, ROWS), pl.ds(r + 1, ROWS)
            prod_y = jnp.zeros((ROWS, width), jnp.float32)
            prod_z = jnp.zeros((ROWS, width), jnp.float32)
            for t in range(steps):
                pt, at = p[t, l, here], a[t, l, here]
                prod_y += (at - a[t, l, after]) * (pt - p[t, l, after])
                prod_z += (at - pltpu.roll(at, width - 1, 1)) * (pt - pltpu.roll(pt, width - 1, 1))
            opened = act[l, here].astype(jnp.float32)
            k1 = k[1, l, here]
            k1_up = k[1, l, after]
            factor = multiplier(code[1, l, here]) * opened * act[l, after].astype(jnp.float32)
            w = jnp.where(row + r < height - 1, weight(prod_y, factor, k1, k1_up), 0.0)
            w_lo = jnp.where(row + r < height - 1, w * k1_up, 0.0)
            tail[pl.ds(r + 8, ROWS)] = w * k1
            log1 = w_lo + tail[pl.ds(r + 7, ROWS)]
            grad[1, l, here] = log1
            k2 = k[2, l, here]
            k2_up = pltpu.roll(k2, width - 1, 1)
            factor = multiplier(code[2, l, here]) * opened * pltpu.roll(opened, width - 1, 1)
            w = jnp.where(lane < width - 1, weight(prod_z, factor, k2, k2_up), 0.0)
            log2 = w * k2_up + pltpu.roll(w * k2, 1, 1)
            grad[2, l, here] = log2
            return total + fold(log1) + fold(log2)

        total = lax.fori_loop(0, blocks, block, total)

        def cross(b, total):
            here = pl.ds(pl.multiple_of(b * ROWS, ROWS), ROWS)
            prod = jnp.zeros((ROWS, width), jnp.float32)
            for t in range(steps):
                prod += (a[t, l, here] - a[t, l + 1, here]) * (p[t, l, here] - p[t, l + 1, here])
            k0, k0_up = k[0, l, here], k[0, l + 1, here]
            factor = multiplier(code[0, l, here]) * (act[l, here] * act[l + 1, here]).astype(jnp.float32)
            w = weight(prod, factor, k0, k0_up)
            log0 = grad[0, l, here] + w * k0_up
            grad[0, l, here] = log0
            grad[0, l + 1, here] = w * k0
            return total + jnp.where(l > 0, 1.0, 0.0) * fold(log0)

        return lax.cond(l < last, lambda total: lax.fori_loop(0, blocks, cross, total), lambda total: total, total)

    total = lax.fori_loop(0, layers, layer, jnp.zeros((8, width), jnp.float32))
    for i in range(layers - 1, len(rounds) + 1):
        turn(i)

    acc[...] = total + jnp.where(me == 0, 1.0, 0.0) * fold(grad[0, 0])

    @pl.when(me < n - 1)
    def _():
        halo_k.wait_recv()
        for c in range(blocks):
            for copy in halo_pa(c):
                copy.wait_recv()
            here = pl.ds(c * ROWS, ROWS)
            prod = jnp.zeros((ROWS, width), jnp.float32)
            for t in range(steps):
                prod += (a[t, last, here] - halo_a[t, here]) * (p[t, last, here] - halo_p[t, here])
            k0, g_up = k[0, last, here], halo_g[here]
            factor = multiplier(code[0, last, here]) * act[last, here].astype(jnp.float32)
            w = weight(prod, factor, k0, g_up)
            w_up = w * k0
            ret_out[here] = w_up
            grad[0, last, here] = grad[0, last, here] + w * g_up
            if c < blocks - 1:
                returned(c).start()
            else:
                halo_first.wait_recv()
                acc[...] = acc[...] + fold(halo_own[...] + w_up)

    def take_back(c):
        here = pl.ds(c * ROWS, ROWS)
        returned(c).wait_recv()
        log0 = grad[0, 0, here] + ret_in[here]
        grad[0, 0, here] = log0
        return fold(log0)

    @pl.when(me > 0)
    def _():
        halo_first.wait_send()
        for c in range(blocks - 1):
            acc[...] = acc[...] + take_back(c)

    mine = jnp.sum(acc[...] + fold(grad[0, last]), axis=0, keepdims=True)
    part[...] = mine

    def to_peer(j):
        return pltpu.make_async_remote_copy(
            src_ref=part, dst_ref=parts.at[j - 1], send_sem=part_send.at[j - 1], recv_sem=part_recv.at[j - 1],
            device_id={"gx": lax.rem(me + j, n)}, device_id_type=MESH)

    def send(j, carry):
        to_peer(j).start()
        return carry

    def receive(j, carry):
        to_peer(j).wait_recv()
        return carry

    lax.fori_loop(1, n, send, 0)

    @pl.when(me < n - 1)
    def _():
        returned(blocks - 1).start()

    @pl.when(me > 0)
    def _():
        take_back(blocks - 1)

    lax.fori_loop(1, n, receive, 0)
    whole = jnp.sum(jnp.sum(parts[...], axis=0) + mine, keepdims=True)
    scale = jnp.broadcast_to(lax.rsqrt(whole / entries + epsilon), (ROWS, width))

    def normalize(i, carry):
        here = pl.ds(pl.multiple_of(i * ROWS, ROWS), ROWS)
        for d in range(3):
            for l in range(layers):
                grad[d, l, here] = grad[d, l, here] * scale
        return carry

    lax.fori_loop(0, blocks, normalize, 0)

    def drain(j, carry):
        to_peer(j).wait_send()
        return carry

    lax.fori_loop(1, n, drain, 0)

    @pl.when(me > 0)
    def _():
        halo_k.wait_send()
        for c in range(blocks):
            for copy in halo_pa(c):
                copy.wait_send()

    @pl.when(me < n - 1)
    def _():
        for c in range(blocks):
            returned(c).wait_send()


def local(pressure, adjoint, permeability, active, fault_codes):
    n = lax.axis_size("gx")
    steps, layers, height, width = pressure.shape
    blocks = height // ROWS
    entries = 3 * layers * n * height * width
    f32 = jnp.float32
    padded = height + PAD
    dma = pltpu.SemaphoreType.DMA
    return pl.pallas_call(
        functools.partial(kernel, n, entries),
        out_shape=pltpu.VMEM((3, layers, height, width), f32),
        in_specs=[pl.BlockSpec(memory_space=pltpu.HBM)] * 5,
        out_specs=pl.BlockSpec(memory_space=pltpu.VMEM),
        scratch_shapes=[
            pltpu.VMEM((steps, layers, padded, width), f32),
            pltpu.VMEM((steps, layers, padded, width), f32),
            pltpu.VMEM((3, layers, padded, width), f32),
            pltpu.VMEM((layers, padded, width), jnp.int32),
            pltpu.VMEM((3, layers, height, width), jnp.int32),
            pltpu.VMEM((steps, height, width), f32),
            pltpu.VMEM((steps, height, width), f32),
            pltpu.VMEM((height, width), f32),
            pltpu.VMEM((ROWS, width), f32),
            pltpu.VMEM((height, width), f32),
            pltpu.VMEM((height, width), f32),
            pltpu.VMEM((height, width), f32),
            pltpu.VMEM((padded, width), f32),
            pltpu.VMEM((8, width), f32),
            pltpu.VMEM((1, width), f32),
            pltpu.VMEM((n - 1, 1, width), f32),
            dma((5, layers)),
            dma((2 * blocks + 2,)),
            dma((2 * blocks + 2,)),
            dma((blocks,)),
            dma((blocks,)),
            dma((n - 1,)),
            dma((n - 1,)),
            pltpu.SemaphoreType.REGULAR((len(distances(n)) + 1,)),
        ],
        compiler_params=pltpu.CompilerParams(collective_id=0, has_side_effects=True, vmem_limit_bytes=GRANT),
        cost_estimate=pl.CostEstimate(flops=100_000_000, bytes_accessed=12_000_000, transcendentals=0),
    )(pressure, adjoint, permeability, active, fault_codes)


def solution(mesh):
    split = ("groups", "gx")
    placed = (P(None, split), P(None, split), P(None, split), P(split), P(None, split))
    return jax.shard_map(local, mesh=mesh, in_specs=placed, out_specs=P(None, split), check_vma=False)
```
